256 devices in a mesh: row: 16 (over y, z_hi), col: 16 (over x, z_lo, core).
Axes of the slice: x: 4, y: 4, z: 8 (z_hi: 4, z_lo: 2; z = z_hi * 2 + z_lo), core: 2. Of those that a mesh axis runs over, the one named last changes fastest.
Arguments:
- rep_a: bfloat16 [8192, 512], P(('row', 'col')), may hold values from -100 to 100
- val_a: bfloat16 [8192, 512], P(('row', 'col')), may hold values from -6 to 6
- rep_b: bfloat16 [16384, 512], P(('row', 'col')), may hold values from -18 to 18
- val_b: bfloat16 [16384, 512], P(('row', 'col')), may hold values from -6 to 6
Outputs:
- mixed_a: float32 [8192, 512], P(('row', 'col'))
- mixed_b: float32 [16384, 512], P(('row', 'col'))
The draws below stay inside these ranges and needn't reach their ends.
All inputs are finite; a program needn't handle non-finite values.
Results may differ from the reference program's by a relative error of at most 0.0015.
Values may be sent and summed in bfloat16 or wider, within the bound.
No kernel may reach another device: no remote copies, remote signals or barrier semaphores. Data moves between devices by JAX's collectives and lax.ppermute only.
A program may use at most 64 MiB of HBM per device.

```python
import math
import jax
import jax.numpy as jnp
from jax import lax

HEADS = 4
HEAD = 128
D = 512
NA = 8192
NB = 16384


def paired_sets(key):
    base = jax.random.fold_in(key, 7001)
    key_first, key_second = jax.random.split(base, 2)
    first_set = jnp.clip(jax.random.normal(key_first, (NA, D), jnp.float32), -6.0, 6.0)
    second_set = 2.8 * jnp.clip(jax.random.normal(key_second, (NB, D), jnp.float32), -6.0, 6.0)
    return (first_set, second_set)


def draw_rep_a(key, part):
    return paired_sets(key)[0].astype(jnp.bfloat16)


def draw_rep_b(key, part):
    return paired_sets(key)[1].astype(jnp.bfloat16)


def steps_of(own_key, dims, cuts, low, largest):
    def one(position, blocks):
        draws = jax.random.uniform(jax.random.fold_in(jax.random.fold_in(own_key, 6), position), (blocks,), jnp.float32, low / len(cuts), largest / len(cuts))
        return jnp.repeat(jnp.exp(draws), dims[position] // blocks).reshape((-1,) + (1,) * (len(dims) - position - 1))

    loudness = one(*cuts[0])
    for cut in cuts[1:]:
        loudness = loudness * one(*cut)
    return loudness


def scatter_about(key, dims, scale, bound, cuts=(), held_as=jnp.bfloat16):
    drawn = jax.random.normal(key, dims, jnp.float32) * scale
    if len(cuts) > 0:
        drawn = steps_of(key, dims, cuts, -0.22, 0.18) * drawn
    return jnp.clip(drawn, min=-bound, max=bound).astype(held_as)


def setup_inputs(seed: int = 0) -> dict:
    keys = jax.random.split(jax.random.key(seed), 5)
    return {
        "rep_a": draw_rep_a(jax.random.fold_in(keys[4], 71), 0),
        "val_a": scatter_about(keys[1], (NA, D), 1.0, 6.0, ((0, 256),)),
        "rep_b": draw_rep_b(jax.random.fold_in(keys[4], 71), 0),
        "val_b": scatter_about(keys[3], (NB, D), 1.0, 6.0, ((0, 256),)),
    }


def attend(queries, key_rows, value_rows):
    count = queries.shape[0]
    span_rows = math.gcd(512, count)
    inv_root = HEAD ** -0.5

    def one_block(query_block):
        pieces = []
        for head in range(HEADS):
            lower = head * HEAD
            logits = jnp.dot(query_block[:, lower:lower + HEAD], key_rows[:, lower:lower + HEAD].T, preferred_element_type=jnp.float32) * inv_root
            row_peak = jnp.max(logits, axis=1)
            weights = jnp.exp(logits - row_peak[:, None])
            totals = jnp.sum(weights, axis=1)
            numerator = jnp.dot(weights.astype(jnp.bfloat16), value_rows[:, lower:lower + HEAD], preferred_element_type=jnp.float32)
            pieces.append(numerator / totals[:, None])
        return jnp.concatenate(pieces, axis=1)

    grouped = queries.reshape(count // span_rows, span_rows, queries.shape[1])
    return lax.map(one_block, grouped).reshape(count, HEADS * HEAD)


def reference(rep_a, val_a, rep_b, val_b):
    return attend(rep_a, rep_b, val_b), attend(rep_b, rep_a, val_a)
```

```python
import functools

import jax
import jax.numpy as jnp
from jax import lax
from jax.experimental import pallas as pl
from jax.experimental.pallas import tpu as pltpu
from jax.sharding import Mesh
from jax.sharding import PartitionSpec as P


HEADS = 4
HEAD = 128
SCALE = HEAD**-0.5 * 1.4426950408889634
LANES = 128
STATS = 16
AXES = ("y", "z_hi", "x", "z_lo", "core")
X, Y, Z, CORE = ("x",), ("y",), ("z_hi", "z_lo"), ("core",)
VMEM = pl.BlockSpec(memory_space=pltpu.VMEM)
SMEM = pl.BlockSpec(memory_space=pltpu.SMEM)
PARAMS = pltpu.CompilerParams(vmem_limit_bytes=40 * 1024 * 1024)


def swap(value, axes, k):
    size = lax.axis_size(axes)
    return lax.ppermute(value, axes, [(i, i ^ k) for i in range(size)])


def exchange(blocks, axes):
    return [blocks[0]] + [swap(b, axes, k) for k, b in enumerate(blocks) if k]


def gather(block, axes):
    return exchange([block] * lax.axis_size(axes), axes)


def split_heads(place, rep_a, val_a, rep_b, val_b, *outs):
    for k, out in enumerate(outs):
        lanes = pl.ds(pl.multiple_of((place[0] ^ k) * HEAD, HEAD), HEAD)
        at = 0
        for source in (rep_a, val_a, rep_b, val_b):
            rows = source.shape[0]
            out[at : at + rows, :] = source[:, lanes]
            at += rows


def join_heads(place, *refs):
    blocks, (out_a, out_b) = refs[:-2], refs[-2:]
    rows_a = out_a.shape[0]
    for k, block in enumerate(blocks):
        lanes = pl.ds(pl.multiple_of((place[0] ^ k) * HEAD, HEAD), HEAD)
        out_a[:, lanes] = block[:rows_a, :]
        out_b[:, lanes] = block[rows_a:, :]


def attend(span, n_own, q_refs, kv_refs, out_refs, scores):
    keys = []
    for ref in kv_refs:
        for at in range(0, ref.shape[0], 2 * span):
            keys.append((ref, at))
    for q_ref, out_ref in zip(q_refs, out_refs):
        rows = q_ref.shape[0] // 2
        queries = q_ref[:rows, :]
        top = None
        for j, (ref, at) in enumerate(keys):
            logits = lax.dot_general(
                queries, ref[at : at + span, :], (((1,), (1,)), ((), ())), preferred_element_type=jnp.float32
            )
            scores[:rows, j * span : (j + 1) * span] = logits
            for c in range(0, span, LANES):
                part = logits[:, c : c + LANES]
                top = part if top is None else jnp.maximum(top, part)
        peak = jnp.max(top, axis=1, keepdims=True) * SCALE
        total, number = None, None
        for j, (ref, at) in enumerate(keys):
            weights = jnp.exp2(scores[:rows, j * span : (j + 1) * span] * SCALE - peak)
            for c in range(0, span, LANES):
                part = weights[:, c : c + LANES]
                total = part if total is None else total + part
            part = jnp.dot(
                weights.astype(jnp.bfloat16), ref[at + span : at + 2 * span, :], preferred_element_type=jnp.float32
            )
            number = part if number is None else number + part
        total = jnp.sum(total, axis=1, keepdims=True)
        out_ref[:rows, :] = (number / total).astype(out_ref.dtype)
        level = jnp.broadcast_to(peak + jnp.log2(total), (rows, LANES))
        for c in range(rows // LANES):
            line = jnp.transpose(level[c * LANES : (c + 1) * LANES, :])[:STATS, :]
            first = line.astype(jnp.bfloat16).astype(jnp.float32)
            second = (line - first).astype(jnp.bfloat16).astype(jnp.float32)
            third = line - first - second
            row = lax.broadcasted_iota(jnp.int32, (STATS, LANES), 0)
            pieces = jnp.where(row == 0, first, jnp.where(row == 1, second, jnp.where(row == 2, third, 0.0)))
            out_ref[rows + c * STATS : rows + (c + 1) * STATS, :] = pieces.astype(out_ref.dtype)


def attend_kernel(span, n_q, n_kv, *refs):
    attend(span, n_q, refs[:n_q], refs[n_q : n_q + n_kv], refs[n_q + n_kv : 2 * n_q + n_kv], refs[-1])


def attention(q_blocks, kv_stacks, span):
    rows = q_blocks[0].shape[0] // 2
    size = rows + STATS * (rows // LANES)
    keys = sum(s.shape[0] for s in kv_stacks) // 2
    out = jax.ShapeDtypeStruct((size, HEAD), jnp.float32)
    n_q, n_kv = len(q_blocks), len(kv_stacks)
    flops = 4 * n_q * rows * keys * HEAD
    return pl.pallas_call(
        functools.partial(attend_kernel, span, n_q, n_kv),
        out_shape=[out] * n_q,
        in_specs=[VMEM] * (n_q + n_kv),
        out_specs=[VMEM] * n_q,
        scratch_shapes=[pltpu.VMEM((rows, keys), jnp.float32)],
        compiler_params=PARAMS,
        cost_estimate=pl.CostEstimate(flops=flops, bytes_accessed=0, transcendentals=n_q * rows * keys),
    )(*q_blocks, *kv_stacks)


def merged(refs, rows):
    columns = []
    for c in range(rows // LANES):
        at = rows + c * STATS
        levels = [
            jnp.sum(ref[at : at + STATS, :].astype(jnp.float32), axis=0, keepdims=True) for ref in refs
        ]
        top = functools.reduce(jnp.maximum, levels)
        shares = [jnp.exp2(level - top) for level in levels]
        whole = functools.reduce(jnp.add, shares)
        result = None
        for ref, share in zip(refs, shares):
            scale = jnp.transpose(jnp.broadcast_to(share / whole, (LANES, LANES)))
            part = ref[c * LANES : (c + 1) * LANES, :].astype(jnp.float32) * scale
            result = part if result is None else result + part
        columns.append(result)
    return columns


def merge_kernel(n_a, n_b, *refs):
    parts_a, parts_b, outs = refs[:n_a], refs[n_a : n_a + n_b], refs[n_a + n_b :]
    groups = len(outs)
    at = 0
    for parts in (parts_a, parts_b):
        rows = parts[0].shape[0] * LANES // (LANES + STATS)
        whole = merged(parts, rows)
        each = rows // groups
        for k, out in enumerate(outs):
            start = k * each
            column, offset = divmod(start, LANES)
            out[at : at + each, :] = whole[column][offset : offset + each, :]
        at += each


def on_device(rep_a, val_a, rep_b, val_b):
    rows_a, rows_b = rep_a.shape[0], rep_b.shape[0]
    chips = lax.axis_size(X)
    place = lax.axis_index(X).astype(jnp.int32).reshape(1)
    bf16, f32 = jnp.bfloat16, jnp.float32

    message = jax.ShapeDtypeStruct((2 * (rows_a + rows_b), HEAD), bf16)
    sent = pl.pallas_call(
        split_heads, out_shape=[message] * chips, in_specs=[SMEM] + [VMEM] * 4, out_specs=[VMEM] * chips
    )(place, rep_a, val_a, rep_b, val_b)
    took = exchange(sent, X)
    edges = (0, rows_a, 2 * rows_a, 2 * rows_a + rows_b, 2 * (rows_a + rows_b))
    own_a = jnp.concatenate([t[edges[i] : edges[i + 1]] for i in (0, 1) for t in took])
    own_b = jnp.concatenate([t[edges[i] : edges[i + 1]] for i in (2, 3) for t in took])

    blocks_b = gather(own_b, Y)
    blocks_a = gather(own_a, Z)
    all_b = jnp.concatenate(blocks_b)
    other_b = swap(all_b, CORE, 1)
    all_a = jnp.concatenate(blocks_a)
    other_a = swap(all_a, CORE, 1)

    span_b, span_a = own_b.shape[0] // 2, own_a.shape[0] // 2
    part_a = attention(blocks_a, [all_b, other_b], span_b)
    part_b = attention(blocks_b, [all_a, other_a], span_a)
    part_a = [p.astype(f32) for p in exchange([p.astype(jnp.float16) for p in part_a], Z)]
    part_b = [p.astype(f32) for p in exchange([p.astype(jnp.float16) for p in part_b], Y)]

    result = jax.ShapeDtypeStruct((rows_a + rows_b, HEAD), f32)
    done = pl.pallas_call(
        functools.partial(merge_kernel, len(part_a), len(part_b)),
        out_shape=[result] * chips,
        in_specs=[VMEM] * (len(part_a) + len(part_b)),
        out_specs=[VMEM] * chips,
    )(*part_a, *part_b)
    back = exchange(done, X)
    return pl.pallas_call(
        join_heads,
        out_shape=[
            jax.ShapeDtypeStruct((rows_a, HEADS * HEAD), f32),
            jax.ShapeDtypeStruct((rows_b, HEADS * HEAD), f32),
        ],
        in_specs=[SMEM] + [VMEM] * chips,
        out_specs=[VMEM] * 2,
    )(place, *back)


def solution(mesh):
    torus = Mesh(mesh.devices.reshape(4, 4, 4, 2, 2), AXES)
    placed = P(AXES, None)
    return jax.shard_map(
        on_device,
        mesh=torus,
        in_specs=(placed,) * 4,
        out_specs=(placed, placed),
        check_vma=False,
    )
```

```python
import functools

import jax
import jax.numpy as jnp
from jax import lax
from jax.experimental import pallas as pl
from jax.experimental.pallas import tpu as pltpu
from jax.sharding import Mesh
from jax.sharding import PartitionSpec as P


HEADS = 4
HEAD = 128
SCALE = HEAD**-0.5 * 1.4426950408889634
LANES = 128
STATS = 16
AXES = ("y", "z_hi", "x", "z_lo", "core")
X, Y, FAR, NEAR, CORE = ("x",), ("y",), ("z_hi",), ("z_lo",), ("core",)
VMEM = pl.BlockSpec(memory_space=pltpu.VMEM)
SMEM = pl.BlockSpec(memory_space=pltpu.SMEM)
PARAMS = pltpu.CompilerParams(vmem_limit_bytes=24 * 1024 * 1024)
SMALL = pltpu.CompilerParams(vmem_limit_bytes=8 * 1024 * 1024)


def swap(value, axes, k):
    size = lax.axis_size(axes)
    return lax.ppermute(value, axes, [(i, i ^ k) for i in range(size)])


def exchange(blocks, axes):
    return [blocks[0]] + [swap(b, axes, k) for k, b in enumerate(blocks) if k]


def gather(block, axes):
    return exchange([block] * lax.axis_size(axes), axes)


def split_heads(place, rep_a, val_a, rep_b, val_b, *outs):
    for k, out in enumerate(outs):
        lanes = pl.ds(pl.multiple_of((place[0] ^ k) * HEAD, HEAD), HEAD)
        at = 0
        for source in (rep_a, val_a, rep_b, val_b):
            rows = source.shape[0]
            out[at : at + rows, :] = source[:, lanes]
            at += rows


def join_heads(place, *refs):
    blocks, (out_a, out_b) = refs[:-2], refs[-2:]
    rows_a = out_a.shape[0]
    for k, block in enumerate(blocks):
        lanes = pl.ds(pl.multiple_of((place[0] ^ k) * HEAD, HEAD), HEAD)
        out_a[:, lanes] = block[:rows_a, :]
        out_b[:, lanes] = block[rows_a:, :]


def attend(span, n_own, q_refs, kv_refs, out_refs, scores):
    keys = []
    for ref in kv_refs:
        for at in range(0, ref.shape[0], 2 * span):
            keys.append((ref, at))
    rows = scores.shape[0]
    for q_whole, out_whole, i in [(q, o, i) for q, o in zip(q_refs, out_refs) for i in range(q.shape[0] // (2 * rows))]:
        size = out_whole.shape[0] * 2 * rows // q_whole.shape[0]
        out_ref = out_whole.at[i * size : (i + 1) * size]
        queries = q_whole[2 * rows * i : 2 * rows * i + rows, :]
        top = None
        for j, (ref, at) in enumerate(keys):
            logits = lax.dot_general(
                queries, ref[at : at + span, :], (((1,), (1,)), ((), ())), preferred_element_type=jnp.float32
            )
            scores[:rows, j * span : (j + 1) * span] = logits
            for c in range(0, span, LANES):
                part = logits[:, c : c + LANES]
                top = part if top is None else jnp.maximum(top, part)
        peak = jnp.max(top, axis=1, keepdims=True) * SCALE
        total, number = None, None
        for j, (ref, at) in enumerate(keys):
            weights = jnp.exp2(scores[:rows, j * span : (j + 1) * span] * SCALE - peak)
            for c in range(0, span, LANES):
                part = weights[:, c : c + LANES]
                total = part if total is None else total + part
            part = jnp.dot(
                weights.astype(jnp.bfloat16), ref[at + span : at + 2 * span, :], preferred_element_type=jnp.float32
            )
            number = part if number is None else number + part
        total = jnp.sum(total, axis=1, keepdims=True)
        out_ref[:rows, :] = (number / total).astype(out_ref.dtype)
        level = jnp.broadcast_to(peak + jnp.log2(total), (rows, LANES))
        for c in range(rows // LANES):
            line = jnp.transpose(level[c * LANES : (c + 1) * LANES, :])[:STATS, :]
            first = line.astype(jnp.bfloat16).astype(jnp.float32)
            second = (line - first).astype(jnp.bfloat16).astype(jnp.float32)
            third = line - first - second
            row = lax.broadcasted_iota(jnp.int32, (STATS, LANES), 0)
            pieces = jnp.where(row == 0, first, jnp.where(row == 1, second, jnp.where(row == 2, third, 0.0)))
            out_ref[rows + c * STATS : rows + (c + 1) * STATS, :] = pieces.astype(out_ref.dtype)


def attend_kernel(span, n_q, n_kv, *refs):
    attend(span, n_q, refs[:n_q], refs[n_q : n_q + n_kv], refs[n_q + n_kv : 2 * n_q + n_kv], refs[-1])


def attention(q_blocks, each, kv_stacks, span):
    rows = q_blocks[0].shape[0] // (2 * each)
    size = each * (rows + STATS * (rows // LANES))
    keys = sum(s.shape[0] for s in kv_stacks) // 2
    out = jax.ShapeDtypeStruct((size, HEAD), jnp.float32)
    n_q, n_kv = len(q_blocks), len(kv_stacks)
    flops = 4 * n_q * each * rows * keys * HEAD
    return pl.pallas_call(
        functools.partial(attend_kernel, span, n_q, n_kv),
        out_shape=[out] * n_q,
        in_specs=[VMEM] * (n_q + n_kv),
        out_specs=[VMEM] * n_q,
        scratch_shapes=[pltpu.VMEM((rows, keys), jnp.float32)],
        compiler_params=PARAMS,
        cost_estimate=pl.CostEstimate(flops=flops, bytes_accessed=0, transcendentals=n_q * each * rows * keys),
    )(*q_blocks, *kv_stacks)


def merged(refs, rows):
    refs = [r.at[i : i + rows + STATS * (rows // LANES)] for r in refs for i in range(0, r.shape[0], rows + STATS * (rows // LANES))]
    columns = []
    for c in range(rows // LANES):
        at = rows + c * STATS
        levels = [
            jnp.sum(ref[at : at + STATS, :].astype(jnp.float32), axis=0, keepdims=True) for ref in refs
        ]
        top = functools.reduce(jnp.maximum, levels)
        shares = [jnp.exp2(level - top) for level in levels]
        whole = functools.reduce(jnp.add, shares)
        result = None
        for ref, share in zip(refs, shares):
            scale = jnp.transpose(jnp.broadcast_to(share / whole, (LANES, LANES)))
            part = ref[c * LANES : (c + 1) * LANES, :].astype(jnp.float32) * scale
            result = part if result is None else result + part
        columns.append(result)
    return columns


def merge_kernel(n_a, n_b, rows_of, *refs):
    parts_a, parts_b, outs = refs[:n_a], refs[n_a : n_a + n_b], refs[n_a + n_b :]
    groups = len(outs)
    at = 0
    for parts, rows in zip((parts_a, parts_b), rows_of):
        whole = merged(parts, rows)
        each = rows // groups
        for k, out in enumerate(outs):
            start = k * each
            column, offset = divmod(start, LANES)
            out[at : at + each, :] = whole[column][offset : offset + each, :]
        at += each


def on_device(rep_a, val_a, rep_b, val_b):
    rows_a, rows_b = rep_a.shape[0], rep_b.shape[0]
    chips = lax.axis_size(X)
    place = lax.axis_index(X).astype(jnp.int32).reshape(1)
    bf16, f32 = jnp.bfloat16, jnp.float32

    message = jax.ShapeDtypeStruct((2 * (rows_a + rows_b), HEAD), bf16)
    sent = pl.pallas_call(
        split_heads, out_shape=[message] * chips, in_specs=[SMEM] + [VMEM] * 4, out_specs=[VMEM] * chips, compiler_params=SMALL
    )(place, rep_a, val_a, rep_b, val_b)
    took = exchange(sent, X)
    edges = (0, rows_a, 2 * rows_a, 2 * rows_a + rows_b, 2 * (rows_a + rows_b))
    own_a = jnp.concatenate([t[edges[i] : edges[i + 1]] for i in (0, 1) for t in took])
    own_b = jnp.concatenate([t[edges[i] : edges[i + 1]] for i in (2, 3) for t in took])

    pair_a = jnp.concatenate([own_a, swap(own_a, NEAR, 1)])
    blocks_b = gather(own_b, Y)
    pairs_a = gather(pair_a, FAR)
    all_b = jnp.concatenate(blocks_b)
    other_b = swap(all_b, CORE, 1)
    all_a = jnp.concatenate(pairs_a)
    other_a = swap(all_a, CORE, 1)

    span_b, span_a = own_b.shape[0] // 2, own_a.shape[0] // 2
    part_a = attention(pairs_a, 2, [all_b, other_b], span_b)
    part_b = attention(blocks_b, 1, [all_a, other_a], span_a)
    part_b = [p.astype(f32) for p in exchange([p.astype(jnp.float16) for p in part_b], Y)]
    part_a = exchange([p.astype(jnp.float16) for p in part_a], FAR)
    half = part_a[0].shape[0] // 2
    far_a = swap(jnp.concatenate([p[half:] for p in part_a]), NEAR, 1)
    part_a = [p[:half].astype(f32) for p in part_a] + [far_a.astype(f32)]

    result = jax.ShapeDtypeStruct((rows_a + rows_b, HEAD), f32)
    done = pl.pallas_call(
        functools.partial(merge_kernel, len(part_a), len(part_b), (chips * rows_a, chips * rows_b)),
        out_shape=[result] * chips,
        in_specs=[VMEM] * (len(part_a) + len(part_b)),
        out_specs=[VMEM] * chips,
        compiler_params=SMALL,
    )(*part_a, *part_b)
    back = exchange(done, X)
    return pl.pallas_call(
        join_heads,
        out_shape=[
            jax.ShapeDtypeStruct((rows_a, HEADS * HEAD), f32),
            jax.ShapeDtypeStruct((rows_b, HEADS * HEAD), f32),
        ],
        in_specs=[SMEM] + [VMEM] * chips,
        out_specs=[VMEM] * 2,
        compiler_params=SMALL,
    )(place, *back)


def solution(mesh):
    torus = Mesh(mesh.devices.reshape(4, 4, 4, 2, 2), AXES)
    placed = P(AXES, None)
    return jax.shard_map(
        on_device,
        mesh=torus,
        in_specs=(placed,) * 4,
        out_specs=(placed, placed),
        check_vma=False,
    )
```

```python
import functools

import jax
import jax.numpy as jnp
from jax import lax
from jax.experimental import pallas as pl
from jax.experimental.pallas import tpu as pltpu
from jax.sharding import Mesh
from jax.sharding import PartitionSpec as P


HEADS = 4
HEAD = 128
SCALE = HEAD**-0.5 * 1.4426950408889634
LANES = 128
STATS = 16
AXES = ("y", "z2", "z1", "x", "z0", "core")
HEAD_AXIS, B_AXIS, A_FAR, A_NEAR, CORE = ("z2", "z1"), ("x",), ("y",), ("z0",), ("core",)
VMEM = pl.BlockSpec(memory_space=pltpu.VMEM)
SMEM = pl.BlockSpec(memory_space=pltpu.SMEM)
HBM = pl.BlockSpec(memory_space=pltpu.HBM)
GROUP = 256
PARAMS = pltpu.CompilerParams(vmem_limit_bytes=24 * 1024 * 1024)
SMALL = pltpu.CompilerParams(vmem_limit_bytes=8 * 1024 * 1024)

WIDE = pltpu.CompilerParams(vmem_limit_bytes=62 * 1024 * 1024)


def swap(value, axes, k):
    size = lax.axis_size(axes)
    return lax.ppermute(value, axes, [(i, i ^ k) for i in range(size)])


def exchange(blocks, axes):
    return [blocks[0]] + [swap(b, axes, k) for k, b in enumerate(blocks) if k]


def gather(block, axes):
    return exchange([block] * lax.axis_size(axes), axes)


def split_heads(place, *refs):
    sources, outs, sems = refs[:4], refs[4:-1], refs[-1]
    copies = []
    for k, out in enumerate(outs):
        lanes = pl.ds(pl.multiple_of((place[0] ^ k) * HEAD, HEAD), HEAD)
        at = 0
        for source in sources:
            rows = source.shape[0]
            copies.append(
                pltpu.make_async_copy(source.at[:, lanes], out.at[at : at + rows], sems.at[len(copies)])
            )
            at += rows
    for copy in copies:
        copy.start()
    for copy in copies:
        copy.wait()


def join_heads(place, *refs):
    blocks, (out_a, out_b) = refs[:-2], refs[-2:]
    rows_a = out_a.shape[0]
    for k, block in enumerate(blocks):
        lanes = pl.ds(pl.multiple_of((place[0] ^ k) * HEAD, HEAD), HEAD)
        out_a[:, lanes] = block[:rows_a, :]
        out_b[:, lanes] = block[rows_a:, :]


def packed(rows):
    return rows + STATS * (rows // LANES)


def stat_rows(level):
    line = jnp.transpose(level)[:STATS, :]
    first = line.astype(jnp.bfloat16).astype(jnp.float32)
    second = (line - first).astype(jnp.bfloat16).astype(jnp.float32)
    third = line - first - second
    row = lax.broadcasted_iota(jnp.int32, (STATS, LANES), 0)
    return jnp.where(row == 0, first, jnp.where(row == 1, second, jnp.where(row == 2, third, 0.0)))


def joined(parts):
    return parts[0] if len(parts) == 1 else jnp.concatenate(parts)


def attend_kernel(rows, span, n_q, n_kv, carried, final, *refs):
    q_refs, kv_refs = refs[:n_q], refs[n_q : n_q + n_kv]
    before = refs[n_q + n_kv : n_q + n_kv + 2 * carried]
    outs, scores = refs[n_q + n_kv + 2 * carried : -1], refs[-1]
    keys = [(ref, at) for ref in kv_refs for at in range(0, ref.shape[0], 2 * span)]
    blocks = [(i, j) for i, ref in enumerate(q_refs) for j in range(ref.shape[0] // (2 * rows))]
    step = GROUP // rows
    for g in range(0, len(blocks), step):
        group = blocks[g : g + step]
        size = rows * len(group)
        queries = joined([q_refs[i][2 * rows * j : 2 * rows * j + rows, :] for i, j in group])
        top = None
        for n, (ref, at) in enumerate(keys):
            logits = lax.dot_general(
                queries, ref[at : at + span, :], (((1,), (1,)), ((), ())), preferred_element_type=jnp.float32
            )
            scores[:size, n * span : (n + 1) * span] = logits
            for c in range(0, span, LANES):
                part = logits[:, c : c + LANES]
                top = part if top is None else jnp.maximum(top, part)
        peak = jnp.max(top, axis=1, keepdims=True) * SCALE
        total, number = None, None
        for n, (ref, at) in enumerate(keys):
            weights = jnp.exp2(scores[:size, n * span : (n + 1) * span] * SCALE - peak)
            for c in range(0, span, LANES):
                part = weights[:, c : c + LANES]
                total = part if total is None else total + part
            part = jnp.dot(
                weights.astype(jnp.bfloat16), ref[at + span : at + 2 * span, :], preferred_element_type=jnp.float32
            )
            number = part if number is None else number + part
        total = jnp.sum(total, axis=1, keepdims=True)
        mean = number / total
        level = jnp.broadcast_to(peak + jnp.log2(total), (size, LANES))
        where = slice(g * rows, g * rows + size)
        if carried:
            old_mean, old_level = before[0][where, :], before[1][where, :]
            best = jnp.maximum(level, old_level)
            new, old = jnp.exp2(level - best), jnp.exp2(old_level - best)
            mean = (mean * new + old_mean * old) / (new + old)
            level = best + jnp.log2(new + old)
        if not final:
            outs[0][where, :] = mean
            outs[1][where, :] = level
            continue
        for n, (i, j) in enumerate(group):
            at = j * packed(rows)
            outs[i][at : at + rows, :] = mean[n * rows : (n + 1) * rows, :]
            for c in range(rows // LANES):
                begin = n * rows + c * LANES
                outs[i][at + rows + c * STATS : at + rows + (c + 1) * STATS, :] = stat_rows(
                    level[begin : begin + LANES, :]
                )


def attention(rows, q_blocks, span, kv_stacks, before=(), final=True):
    heights = [q.shape[0] // 2 for q in q_blocks]
    whole = sum(heights)
    keys = sum(s.shape[0] for s in kv_stacks) // 2
    if final:
        shapes = [(h // rows * packed(rows), HEAD) for h in heights]
    else:
        shapes = [(whole, HEAD), (whole, LANES)]
    n_q, n_kv = len(q_blocks), len(kv_stacks)
    return pl.pallas_call(
        functools.partial(attend_kernel, rows, span, n_q, n_kv, len(before) // 2, final),
        out_shape=[jax.ShapeDtypeStruct(s, jnp.float32) for s in shapes],
        in_specs=[VMEM] * (n_q + n_kv + len(before)),
        out_specs=[VMEM] * len(shapes),
        scratch_shapes=[pltpu.VMEM((GROUP, keys), jnp.float32)],
        compiler_params=PARAMS,
        cost_estimate=pl.CostEstimate(flops=4 * whole * keys * HEAD, bytes_accessed=0, transcendentals=whole * keys),
    )(*q_blocks, *kv_stacks, *before)


def merged(refs, rows):
    parts = [r.at[: packed(rows)] for r in refs]
    columns = []
    for c in range(rows // LANES):
        at = rows + c * STATS
        levels = [jnp.sum(p[at : at + STATS, :], axis=0, keepdims=True) for p in parts]
        top = functools.reduce(jnp.maximum, levels)
        shares = [jnp.exp2(level - top) for level in levels]
        whole = functools.reduce(jnp.add, shares)
        result = None
        for part, share in zip(parts, shares):
            scale = jnp.transpose(jnp.broadcast_to(share / whole, (LANES, LANES)))
            term = part[c * LANES : (c + 1) * LANES, :] * scale
            result = term if result is None else result + term
        columns.append(result)
    return columns


def fold_kernel(rows, *refs):
    parts, out = refs[:-1], refs[-1]
    halves = [p.at[packed(rows) :] for p in parts]
    levels = [jnp.sum(h[rows : rows + STATS, :], axis=0, keepdims=True) for h in halves]
    top = functools.reduce(jnp.maximum, levels)
    shares = [jnp.exp2(level - top) for level in levels]
    whole = functools.reduce(jnp.add, shares)
    result = None
    for half, share in zip(halves, shares):
        term = half[:rows, :] * jnp.transpose(jnp.broadcast_to(share / whole, (LANES, LANES)))
        result = term if result is None else result + term
    out[:rows, :] = result
    out[rows:, :] = stat_rows(jnp.transpose(jnp.broadcast_to(top + jnp.log2(whole), (LANES, LANES))))


def merge_kernel(n_a, n_b, rows_of, *refs):
    parts_a, parts_b, outs = refs[:n_a], refs[n_a : n_a + n_b], refs[n_a + n_b :]
    at = 0
    for parts, rows in zip((parts_a, parts_b), rows_of):
        whole = merged(parts, rows)
        each = rows // len(outs)
        for k, out in enumerate(outs):
            column, offset = divmod(k * each, LANES)
            out[at : at + each, :] = whole[column][offset : offset + each, :]
        at += each


def both_ways(rep_a, val_a, rep_b, val_b):
    rows_a, rows_b = rep_a.shape[0], rep_b.shape[0]
    heads = lax.axis_size(HEAD_AXIS)
    place = lax.axis_index(HEAD_AXIS).astype(jnp.int32).reshape(1)
    bf16, f16, f32 = jnp.bfloat16, jnp.float16, jnp.float32

    message = jax.ShapeDtypeStruct((2 * (rows_a + rows_b), HEAD), bf16)
    sent = pl.pallas_call(
        split_heads,
        out_shape=[message] * heads,
        in_specs=[SMEM] + [HBM] * 4,
        out_specs=[VMEM] * heads,
        scratch_shapes=[pltpu.SemaphoreType.DMA((4 * heads,))],
        compiler_params=WIDE,
    )(place, rep_a, val_a, rep_b, val_b)
    took = exchange(sent, HEAD_AXIS)
    edges = (0, rows_a, 2 * rows_a, 2 * rows_a + rows_b, 2 * (rows_a + rows_b))
    own_a = jnp.concatenate([t[edges[i] : edges[i + 1]] for i in (0, 1) for t in took])
    own_b = jnp.concatenate([t[edges[i] : edges[i + 1]] for i in (2, 3) for t in took])
    span_a, span_b = heads * rows_a, heads * rows_b

    near_a = swap(own_a, A_NEAR, 1)
    blocks_b = gather(own_b, B_AXIS)
    pair_a = jnp.concatenate([own_a, near_a])
    pairs_a = gather(pair_a, A_FAR)
    all_b = jnp.concatenate(blocks_b)
    other_b = swap(all_b, CORE, 1)
    first_a = swap(pair_a, CORE, 1)
    rest_a = jnp.concatenate(pairs_a[1:])
    other_a = swap(rest_a, CORE, 1)

    keys_b = [all_b, other_b]
    part_a = attention(span_a, pairs_a[:1], span_b, keys_b)
    begun = attention(span_b, blocks_b, span_a, [pair_a, first_a], final=False)
    part_a += attention(span_a, pairs_a[1:], span_b, keys_b)
    part_a = [p.astype(f16) for p in part_a]
    part_a, other_a = lax.optimization_barrier((part_a, other_a))
    part_b = attention(span_b, blocks_b, span_a, [rest_a, other_a], before=begun)

    part_a = exchange(part_a, A_FAR)
    part_a = [p.astype(f32) for p in part_a]
    folded = pl.pallas_call(
        functools.partial(fold_kernel, span_a),
        out_shape=jax.ShapeDtypeStruct((packed(span_a), HEAD), f32),
        in_specs=[VMEM] * len(part_a),
        out_specs=VMEM,
        compiler_params=SMALL,
    )(*part_a)
    near_back = swap(folded.astype(f16), A_NEAR, 1)
    part_a = part_a + [near_back.astype(f32)]
    part_b = exchange([p.astype(f16) for p in part_b], B_AXIS)
    part_b = [p.astype(f32) for p in part_b]

    result = jax.ShapeDtypeStruct((rows_a + rows_b, HEAD), f32)
    done = pl.pallas_call(
        functools.partial(merge_kernel, len(part_a), len(part_b), (span_a, span_b)),
        out_shape=[result] * heads,
        in_specs=[VMEM] * (len(part_a) + len(part_b)),
        out_specs=[VMEM] * heads,
        compiler_params=SMALL,
    )(*part_a, *part_b)
    back = [done[0]] + [b.astype(f32) for b in exchange([d.astype(f16) for d in done], HEAD_AXIS)[1:]]
    return pl.pallas_call(
        join_heads,
        out_shape=[
            jax.ShapeDtypeStruct((rows_a, HEADS * HEAD), f32),
            jax.ShapeDtypeStruct((rows_b, HEADS * HEAD), f32),
        ],
        in_specs=[SMEM] + [VMEM] * heads,
        out_specs=[VMEM] * 2,
        compiler_params=SMALL,
    )(place, *back)


def solution(mesh):
    torus = Mesh(mesh.devices.reshape(4, 2, 2, 4, 2, 2), AXES)
    placed = P(AXES, None)
    return jax.shard_map(
        both_ways,
        mesh=torus,
        in_specs=(placed,) * 4,
        out_specs=(placed, placed),
        check_vma=False,
    )
```

```python
import functools

import jax
import jax.numpy as jnp
from jax import lax
from jax.experimental import pallas as pl
from jax.experimental.pallas import tpu as pltpu
from jax.sharding import Mesh
from jax.sharding import PartitionSpec as P


HEADS = 4
HEAD = 128
SCALE = HEAD**-0.5 * 1.4426950408889634
LANES = 128
STATS = 16
AXES = ("y", "z2", "z1", "x", "z0", "core")
HEAD_AXIS, B_AXIS, A_FAR, A_NEAR, CORE = ("z2", "z1"), ("x",), ("y",), ("z0",), ("core",)
VMEM = pl.BlockSpec(memory_space=pltpu.VMEM)
SMEM = pl.BlockSpec(memory_space=pltpu.SMEM)
HBM = pl.BlockSpec(memory_space=pltpu.HBM)
GROUP = 256
PARAMS = pltpu.CompilerParams(vmem_limit_bytes=24 * 1024 * 1024)
SMALL = pltpu.CompilerParams(vmem_limit_bytes=8 * 1024 * 1024)

WIDE = pltpu.CompilerParams(vmem_limit_bytes=62 * 1024 * 1024)


def swap(value, axes, k):
    size = lax.axis_size(axes)
    return lax.ppermute(value, axes, [(i, i ^ k) for i in range(size)])


def exchange(blocks, axes):
    return [blocks[0]] + [swap(b, axes, k) for k, b in enumerate(blocks) if k]


def gather(block, axes):
    return exchange([block] * lax.axis_size(axes), axes)


def split_heads(place, *refs):
    sources, outs, sems = refs[:4], refs[4:-1], refs[-1]
    copies = []
    for k, out in enumerate(outs):
        lanes = pl.ds(pl.multiple_of((place[0] ^ k) * HEAD, HEAD), HEAD)
        at = 0
        for source in sources:
            rows = source.shape[0]
            copies.append(
                pltpu.make_async_copy(source.at[:, lanes], out.at[at : at + rows], sems.at[len(copies)])
            )
            at += rows
    for copy in copies:
        copy.start()
    for copy in copies:
        copy.wait()


def join_heads(place, *refs):
    blocks, (out_a, out_b) = refs[:-2], refs[-2:]
    rows_a = out_a.shape[0]
    for k, block in enumerate(blocks):
        lanes = pl.ds(pl.multiple_of((place[0] ^ k) * HEAD, HEAD), HEAD)
        out_a[:, lanes] = block[:rows_a, :]
        out_b[:, lanes] = block[rows_a:, :]


def packed(rows):
    return rows + STATS * (rows // LANES)


def stat_rows(level):
    line = jnp.transpose(level)[:STATS, :]
    first = line.astype(jnp.bfloat16).astype(jnp.float32)
    second = (line - first).astype(jnp.bfloat16).astype(jnp.float32)
    third = line - first - second
    row = lax.broadcasted_iota(jnp.int32, (STATS, LANES), 0)
    return jnp.where(row == 0, first, jnp.where(row == 1, second, jnp.where(row == 2, third, 0.0)))


def joined(parts):
    return parts[0] if len(parts) == 1 else jnp.concatenate(parts)


def attend_kernel(rows, span, n_q, n_kv, carried, final, *refs):
    q_refs, kv_refs = refs[:n_q], refs[n_q : n_q + n_kv]
    before = refs[n_q + n_kv : n_q + n_kv + 2 * carried]
    outs, scores = refs[n_q + n_kv + 2 * carried : -1], refs[-1]
    keys = [(ref, at) for ref in kv_refs for at in range(0, ref.shape[0], 2 * span)]
    blocks = [(i, j) for i, ref in enumerate(q_refs) for j in range(ref.shape[0] // (2 * rows))]
    step = GROUP // rows
    groups = [blocks[g : g + step] for g in range(0, len(blocks), step)]
    tops = [None] * len(groups)

    def score(g, n):
        queries = joined([q_refs[i][2 * rows * j : 2 * rows * j + rows, :] for i, j in groups[g]])
        ref, at = keys[n]
        logits = lax.dot_general(
            queries, ref[at : at + span, :], (((1,), (1,)), ((), ())), preferred_element_type=jnp.float32
        )
        scores[g % 2, : queries.shape[0], n * span : (n + 1) * span] = logits
        for c in range(0, span, LANES):
            part = logits[:, c : c + LANES]
            tops[g] = part if tops[g] is None else jnp.maximum(tops[g], part)

    for n in range(len(keys)):
        score(0, n)
    for at_group, group in enumerate(groups):
        g, size = at_group * step, rows * len(group)
        peak = jnp.max(tops[at_group], axis=1, keepdims=True) * SCALE
        total, number = None, None
        for n, (ref, at) in enumerate(keys):
            weights = jnp.exp2(scores[at_group % 2, :size, n * span : (n + 1) * span] * SCALE - peak)
            for c in range(0, span, LANES):
                part = weights[:, c : c + LANES]
                total = part if total is None else total + part
            part = jnp.dot(
                weights.astype(jnp.bfloat16), ref[at + span : at + 2 * span, :], preferred_element_type=jnp.float32
            )
            number = part if number is None else number + part
            if at_group + 1 < len(groups):
                score(at_group + 1, n)
        total = jnp.sum(total, axis=1, keepdims=True)
        mean = number / total
        level = jnp.broadcast_to(peak + jnp.log2(total), (size, LANES))
        where = slice(g * rows, g * rows + size)
        if carried:
            old_mean, old_level = before[0][where, :], before[1][where, :]
            best = jnp.maximum(level, old_level)
            new, old = jnp.exp2(level - best), jnp.exp2(old_level - best)
            mean = (mean * new + old_mean * old) / (new + old)
            level = best + jnp.log2(new + old)
        if not final:
            outs[0][where, :] = mean
            outs[1][where, :] = level
            continue
        for n, (i, j) in enumerate(group):
            at = j * packed(rows)
            outs[i][at : at + rows, :] = mean[n * rows : (n + 1) * rows, :]
            for c in range(rows // LANES):
                begin = n * rows + c * LANES
                outs[i][at + rows + c * STATS : at + rows + (c + 1) * STATS, :] = stat_rows(
                    level[begin : begin + LANES, :]
                )


def attention(rows, q_blocks, span, kv_stacks, before=(), final=True):
    heights = [q.shape[0] // 2 for q in q_blocks]
    whole = sum(heights)
    keys = sum(s.shape[0] for s in kv_stacks) // 2
    if final:
        shapes = [(h // rows * packed(rows), HEAD) for h in heights]
    else:
        shapes = [(whole, HEAD), (whole, LANES)]
    n_q, n_kv = len(q_blocks), len(kv_stacks)
    return pl.pallas_call(
        functools.partial(attend_kernel, rows, span, n_q, n_kv, len(before) // 2, final),
        out_shape=[jax.ShapeDtypeStruct(s, jnp.float32) for s in shapes],
        in_specs=[VMEM] * (n_q + n_kv + len(before)),
        out_specs=[VMEM] * len(shapes),
        scratch_shapes=[pltpu.VMEM((2, GROUP, keys), jnp.float32)],
        compiler_params=PARAMS,
        cost_estimate=pl.CostEstimate(flops=4 * whole * keys * HEAD, bytes_accessed=0, transcendentals=whole * keys),
    )(*q_blocks, *kv_stacks, *before)


def merged(refs, rows):
    parts = [r.at[: packed(rows)] for r in refs]
    columns = []
    for c in range(rows // LANES):
        at = rows + c * STATS
        levels = [jnp.sum(p[at : at + STATS, :], axis=0, keepdims=True) for p in parts]
        top = functools.reduce(jnp.maximum, levels)
        shares = [jnp.exp2(level - top) for level in levels]
        whole = functools.reduce(jnp.add, shares)
        result = None
        for part, share in zip(parts, shares):
            scale = jnp.transpose(jnp.broadcast_to(share / whole, (LANES, LANES)))
            term = part[c * LANES : (c + 1) * LANES, :] * scale
            result = term if result is None else result + term
        columns.append(result)
    return columns


def fold_kernel(rows, *refs):
    parts, out = refs[:-1], refs[-1]
    halves = [p.at[packed(rows) :] for p in parts]
    levels = [jnp.sum(h[rows : rows + STATS, :], axis=0, keepdims=True) for h in halves]
    top = functools.reduce(jnp.maximum, levels)
    shares = [jnp.exp2(level - top) for level in levels]
    whole = functools.reduce(jnp.add, shares)
    result = None
    for half, share in zip(halves, shares):
        term = half[:rows, :] * jnp.transpose(jnp.broadcast_to(share / whole, (LANES, LANES)))
        result = term if result is None else result + term
    out[:rows, :] = result
    out[rows:, :] = stat_rows(jnp.transpose(jnp.broadcast_to(top + jnp.log2(whole), (LANES, LANES))))


def merge_kernel(n_a, n_b, rows_of, *refs):
    parts_a, parts_b, outs = refs[:n_a], refs[n_a : n_a + n_b], refs[n_a + n_b :]
    at = 0
    for parts, rows in zip((parts_a, parts_b), rows_of):
        whole = merged(parts, rows)
        each = rows // len(outs)
        for k, out in enumerate(outs):
            column, offset = divmod(k * each, LANES)
            out[at : at + each, :] = whole[column][offset : offset + each, :]
        at += each


def both_ways(rep_a, val_a, rep_b, val_b):
    rows_a, rows_b = rep_a.shape[0], rep_b.shape[0]
    heads = lax.axis_size(HEAD_AXIS)
    place = lax.axis_index(HEAD_AXIS).astype(jnp.int32).reshape(1)
    bf16, f16, f32 = jnp.bfloat16, jnp.float16, jnp.float32

    message = jax.ShapeDtypeStruct((2 * (rows_a + rows_b), HEAD), bf16)
    sent = pl.pallas_call(
        split_heads,
        out_shape=[message] * heads,
        in_specs=[SMEM] + [HBM] * 4,
        out_specs=[VMEM] * heads,
        scratch_shapes=[pltpu.SemaphoreType.DMA((4 * heads,))],
        compiler_params=SMALL,
    )(place, *(pltpu.with_memory_space_constraint(x, pltpu.HBM) for x in (rep_a, val_a, rep_b, val_b)))
    took = exchange(sent, HEAD_AXIS)
    edges = (0, rows_a, 2 * rows_a, 2 * rows_a + rows_b, 2 * (rows_a + rows_b))
    own_a = jnp.concatenate([t[edges[i] : edges[i + 1]] for i in (0, 1) for t in took])
    own_b = jnp.concatenate([t[edges[i] : edges[i + 1]] for i in (2, 3) for t in took])
    span_a, span_b = heads * rows_a, heads * rows_b

    near_a = swap(own_a, A_NEAR, 1)
    blocks_b = gather(own_b, B_AXIS)
    pair_a = jnp.concatenate([own_a, near_a])
    pairs_a = gather(pair_a, A_FAR)
    all_b = jnp.concatenate(blocks_b)
    other_b = swap(all_b, CORE, 1)
    first_a = swap(pair_a, CORE, 1)
    rest_a = jnp.concatenate(pairs_a[1:])
    other_a = swap(rest_a, CORE, 1)

    keys_b = [all_b, other_b]
    part_a = attention(span_a, pairs_a[:1], span_b, keys_b)
    begun = attention(span_b, blocks_b, span_a, [pair_a, first_a], final=False)
    part_a += attention(span_a, pairs_a[1:], span_b, keys_b)
    part_a = [p.astype(f16) for p in part_a]
    part_a, other_a = lax.optimization_barrier((part_a, other_a))
    part_b = attention(span_b, blocks_b, span_a, [rest_a, other_a], before=begun)

    part_a = exchange(part_a, A_FAR)
    part_a = [p.astype(f32) for p in part_a]
    folded = pl.pallas_call(
        functools.partial(fold_kernel, span_a),
        out_shape=jax.ShapeDtypeStruct((packed(span_a), HEAD), f32),
        in_specs=[VMEM] * len(part_a),
        out_specs=VMEM,
        compiler_params=SMALL,
    )(*part_a)
    near_back = swap(folded.astype(f16), A_NEAR, 1)
    part_a = part_a + [near_back.astype(f32)]
    part_b = exchange([p.astype(f16) for p in part_b], B_AXIS)
    part_b = [p.astype(f32) for p in part_b]

    result = jax.ShapeDtypeStruct((rows_a + rows_b, HEAD), f32)
    done = pl.pallas_call(
        functools.partial(merge_kernel, len(part_a), len(part_b), (span_a, span_b)),
        out_shape=[result] * heads,
        in_specs=[VMEM] * (len(part_a) + len(part_b)),
        out_specs=[VMEM] * heads,
        compiler_params=SMALL,
    )(*part_a, *part_b)
    back = [done[0]] + [b.astype(f32) for b in exchange([d.astype(f16) for d in done], HEAD_AXIS)[1:]]
    return pl.pallas_call(
        join_heads,
        out_shape=[
            jax.ShapeDtypeStruct((rows_a, HEADS * HEAD), f32),
            jax.ShapeDtypeStruct((rows_b, HEADS * HEAD), f32),
        ],
        in_specs=[SMEM] + [VMEM] * heads,
        out_specs=[VMEM] * 2,
        compiler_params=SMALL,
    )(place, *back)


def solution(mesh):
    torus = Mesh(mesh.devices.reshape(4, 2, 2, 4, 2, 2), AXES)
    placed = P(AXES, None)
    return jax.shard_map(
        both_ways,
        mesh=torus,
        in_specs=(placed,) * 4,
        out_specs=(placed, placed),
        check_vma=False,
    )
```

```python
import functools

import jax
import jax.numpy as jnp
from jax import lax
from jax.experimental import pallas as pl
from jax.experimental.pallas import tpu as pltpu
from jax.sharding import Mesh
from jax.sharding import PartitionSpec as P


HEADS = 4
HEAD = 128
SCALE = HEAD**-0.5 * 1.4426950408889634
LANES = 128
STATS = 16
AXES = ("y", "z2", "z1", "x", "z0", "core")
HEAD_AXIS, B_AXIS, A_FAR, A_NEAR, CORE = ("z2", "z1"), ("x",), ("y",), ("z0",), ("core",)
VMEM = pl.BlockSpec(memory_space=pltpu.VMEM)
SMEM = pl.BlockSpec(memory_space=pltpu.SMEM)
HBM = pl.BlockSpec(memory_space=pltpu.HBM)
GROUP = 256
CHUNK_A = 1024
PARAMS = pltpu.CompilerParams(vmem_limit_bytes=24 * 1024 * 1024)
SMALL = pltpu.CompilerParams(vmem_limit_bytes=8 * 1024 * 1024)

WIDE = pltpu.CompilerParams(vmem_limit_bytes=62 * 1024 * 1024)


def swap(value, axes, k):
    size = lax.axis_size(axes)
    return lax.ppermute(value, axes, [(i, i ^ k) for i in range(size)])


def exchange(blocks, axes):
    taken = [blocks[0]]
    for k, block in enumerate(blocks[1:], 1):
        taken.append(swap(block, axes, k))
    return taken


def gather(block, axes):
    return exchange([block] * lax.axis_size(axes), axes)


def split_heads(place, *refs):
    sources, outs, sems = refs[:4], refs[4:-1], refs[-1]
    copies = []
    for k, out in enumerate(outs):
        lanes = pl.ds(pl.multiple_of((place[0] ^ k) * HEAD, HEAD), HEAD)
        at = 0
        for source in sources:
            rows = source.shape[0]
            copies.append(
                pltpu.make_async_copy(source.at[:, lanes], out.at[at : at + rows], sems.at[len(copies)])
            )
            at += rows
    for copy in copies:
        copy.start()
    for copy in copies:
        copy.wait()


def join_heads(place, *refs):
    blocks, (out_a, out_b) = refs[:-2], refs[-2:]
    rows_a = out_a.shape[0]
    for k, block in enumerate(blocks):
        lanes = pl.ds(pl.multiple_of((place[0] ^ k) * HEAD, HEAD), HEAD)
        out_a[:, lanes] = block[:rows_a, :]
        out_b[:, lanes] = block[rows_a:, :]


def packed(rows):
    return rows + STATS * (rows // LANES)


def stat_rows(level):
    line = jnp.transpose(level)[:STATS, :]
    first = line.astype(jnp.bfloat16).astype(jnp.float32)
    second = (line - first).astype(jnp.bfloat16).astype(jnp.float32)
    third = line - first - second
    row = lax.broadcasted_iota(jnp.int32, (STATS, LANES), 0)
    return jnp.where(row == 0, first, jnp.where(row == 1, second, jnp.where(row == 2, third, 0.0)))


def joined(parts):
    return parts[0] if len(parts) == 1 else jnp.concatenate(parts)


def attend_kernel(rows, span, chunk_keys, n_q, n_kv, carried, final, *refs):
    q_refs, kv_refs = refs[:n_q], refs[n_q : n_q + n_kv]
    before = refs[n_q + n_kv : n_q + n_kv + 2 * carried]
    outs, scores = refs[n_q + n_kv + 2 * carried : -1], refs[-1]
    keys = [(ref, at) for ref in kv_refs for at in range(0, ref.shape[0], 2 * span)]
    blocks = [(i, j) for i, ref in enumerate(q_refs) for j in range(ref.shape[0] // (2 * rows))]
    step = GROUP // rows
    per = chunk_keys // span
    keys = [keys[n : n + per] for n in range(0, len(keys), per)]
    starts = [n * chunk_keys for n in range(len(keys))]
    groups = [blocks[g : g + step] for g in range(0, len(blocks), step)]
    tops = [None] * len(groups)

    def score(g, n):
        queries = joined([q_refs[i][2 * rows * j : 2 * rows * j + rows, :] for i, j in groups[g]])
        piece = joined([ref[at : at + span, :] for ref, at in keys[n]])
        logits = lax.dot_general(queries, piece, (((1,), (1,)), ((), ())), preferred_element_type=jnp.float32)
        scores[g % 2, : queries.shape[0], starts[n] : starts[n] + logits.shape[1]] = logits
        for c in range(0, logits.shape[1], LANES):
            part = logits[:, c : c + LANES]
            tops[g] = part if tops[g] is None else jnp.maximum(tops[g], part)

    for n in range(len(keys)):
        score(0, n)
    for at_group, group in enumerate(groups):
        g, size = at_group * step, rows * len(group)
        peak = jnp.max(tops[at_group], axis=1, keepdims=True) * SCALE
        total, number = None, None
        for n, chunk in enumerate(keys):
            piece = joined([ref[at + span : at + 2 * span, :] for ref, at in chunk])
            weights = jnp.exp2(scores[at_group % 2, :size, starts[n] : starts[n] + piece.shape[0]] * SCALE - peak)
            for c in range(0, piece.shape[0], LANES):
                part = weights[:, c : c + LANES]
                total = part if total is None else total + part
            part = jnp.dot(weights.astype(jnp.bfloat16), piece, preferred_element_type=jnp.float32)
            number = part if number is None else number + part
            if at_group + 1 < len(groups):
                score(at_group + 1, n)
        total = jnp.sum(total, axis=1, keepdims=True)
        mean = number / total
        level = jnp.broadcast_to(peak + jnp.log2(total), (size, LANES))
        where = slice(g * rows, g * rows + size)
        if carried:
            old_mean, old_level = before[0][where, :], before[1][where, :]
            best = jnp.maximum(level, old_level)
            new, old = jnp.exp2(level - best), jnp.exp2(old_level - best)
            mean = (mean * new + old_mean * old) / (new + old)
            level = best + jnp.log2(new + old)
        if not final:
            outs[0][where, :] = mean
            outs[1][where, :] = level
            continue
        for n, (i, j) in enumerate(group):
            at = j * packed(rows)
            outs[i][at : at + rows, :] = mean[n * rows : (n + 1) * rows, :]
            for c in range(rows // LANES):
                begin = n * rows + c * LANES
                outs[i][at + rows + c * STATS : at + rows + (c + 1) * STATS, :] = stat_rows(
                    level[begin : begin + LANES, :]
                )


def attention(rows, q_blocks, span, kv_stacks, before=(), final=True, chunk=None):
    heights = [q.shape[0] // 2 for q in q_blocks]
    whole = sum(heights)
    keys = sum(s.shape[0] for s in kv_stacks) // 2
    if final:
        shapes = [(h // rows * packed(rows), HEAD) for h in heights]
    else:
        shapes = [(whole, HEAD), (whole, LANES)]
    n_q, n_kv = len(q_blocks), len(kv_stacks)
    return pl.pallas_call(
        functools.partial(attend_kernel, rows, span, chunk or span, n_q, n_kv, len(before) // 2, final),
        out_shape=[jax.ShapeDtypeStruct(s, jnp.float32) for s in shapes],
        in_specs=[VMEM] * (n_q + n_kv + len(before)),
        out_specs=[VMEM] * len(shapes),
        scratch_shapes=[pltpu.VMEM((2, GROUP, keys), jnp.float32)],
        compiler_params=PARAMS,
        cost_estimate=pl.CostEstimate(flops=4 * whole * keys * HEAD, bytes_accessed=0, transcendentals=whole * keys),
    )(*q_blocks, *kv_stacks, *before)


def merged(refs, rows):
    parts = [r.at[: packed(rows)] for r in refs]
    columns = []
    for c in range(rows // LANES):
        at = rows + c * STATS
        levels = [jnp.sum(p[at : at + STATS, :], axis=0, keepdims=True) for p in parts]
        top = functools.reduce(jnp.maximum, levels)
        shares = [jnp.exp2(level - top) for level in levels]
        whole = functools.reduce(jnp.add, shares)
        result = None
        for part, share in zip(parts, shares):
            scale = jnp.transpose(jnp.broadcast_to(share / whole, (LANES, LANES)))
            term = part[c * LANES : (c + 1) * LANES, :] * scale
            result = term if result is None else result + term
        columns.append(result)
    return columns


def fold_kernel(rows, *refs):
    parts, out = refs[:-1], refs[-1]
    halves = [p.at[packed(rows) :] for p in parts]
    levels = [jnp.sum(h[rows : rows + STATS, :], axis=0, keepdims=True) for h in halves]
    top = functools.reduce(jnp.maximum, levels)
    shares = [jnp.exp2(level - top) for level in levels]
    whole = functools.reduce(jnp.add, shares)
    result = None
    for half, share in zip(halves, shares):
        term = half[:rows, :] * jnp.transpose(jnp.broadcast_to(share / whole, (LANES, LANES)))
        result = term if result is None else result + term
    out[:rows, :] = result
    out[rows:, :] = stat_rows(jnp.transpose(jnp.broadcast_to(top + jnp.log2(whole), (LANES, LANES))))


def merge_kernel(n_a, n_b, rows_of, *refs):
    parts_a, parts_b, outs = refs[:n_a], refs[n_a : n_a + n_b], refs[n_a + n_b :]
    at = 0
    for parts, rows in zip((parts_a, parts_b), rows_of):
        whole = merged(parts, rows)
        each = rows // len(outs)
        for k, out in enumerate(outs):
            column, offset = divmod(k * each, LANES)
            out[at : at + each, :] = whole[column][offset : offset + each, :]
        at += each


def both_ways(rep_a, val_a, rep_b, val_b):
    rows_a, rows_b = rep_a.shape[0], rep_b.shape[0]
    heads = lax.axis_size(HEAD_AXIS)
    place = lax.axis_index(HEAD_AXIS).astype(jnp.int32).reshape(1)
    bf16, f16, f32 = jnp.bfloat16, jnp.float16, jnp.float32

    message = jax.ShapeDtypeStruct((2 * (rows_a + rows_b), HEAD), bf16)
    sent = pl.pallas_call(
        split_heads,
        out_shape=[message] * heads,
        in_specs=[SMEM] + [HBM] * 4,
        out_specs=[VMEM] * heads,
        scratch_shapes=[pltpu.SemaphoreType.DMA((4 * heads,))],
        compiler_params=SMALL,
    )(place, *(pltpu.with_memory_space_constraint(x, pltpu.HBM) for x in (rep_a, val_a, rep_b, val_b)))
    took = exchange(sent, HEAD_AXIS)
    edges = (0, rows_a, 2 * rows_a, 2 * rows_a + rows_b, 2 * (rows_a + rows_b))
    own_a = jnp.concatenate([t[edges[i] : edges[i + 1]] for i in (0, 1) for t in took])
    own_b = jnp.concatenate([t[edges[i] : edges[i + 1]] for i in (2, 3) for t in took])
    span_a, span_b = heads * rows_a, heads * rows_b

    near_a = swap(own_a, A_NEAR, 1)
    blocks_b = gather(own_b, B_AXIS)
    pair_a = jnp.concatenate([own_a, near_a])
    pairs_a = gather(pair_a, A_FAR)
    all_b = jnp.concatenate(blocks_b)
    other_b = swap(all_b, CORE, 1)
    first_a = swap(pair_a, CORE, 1)
    rest_a = jnp.concatenate(pairs_a[1:])
    other_a = swap(rest_a, CORE, 1)

    keys_b = [all_b, other_b]
    part_a = attention(span_a, pairs_a[:1], span_b, keys_b, chunk=CHUNK_A)
    begun = attention(span_b, blocks_b, span_a, [pair_a, first_a], final=False)
    part_a += attention(span_a, pairs_a[1:], span_b, keys_b, chunk=CHUNK_A)
    part_a = [p.astype(f16) for p in part_a]
    part_a, other_a = lax.optimization_barrier((part_a, other_a))
    part_b = attention(span_b, blocks_b, span_a, [rest_a, other_a], before=begun)

    part_a = exchange(part_a, A_FAR)
    part_a = [p.astype(f32) for p in part_a]
    folded = pl.pallas_call(
        functools.partial(fold_kernel, span_a),
        out_shape=jax.ShapeDtypeStruct((packed(span_a), HEAD), f32),
        in_specs=[VMEM] * len(part_a),
        out_specs=VMEM,
        compiler_params=SMALL,
    )(*part_a)
    near_back = swap(folded.astype(f16), A_NEAR, 1)
    part_a = part_a + [near_back.astype(f32)]
    part_b = exchange([p.astype(f16) for p in part_b], B_AXIS)
    part_b = [p.astype(f32) for p in part_b]

    result = jax.ShapeDtypeStruct((rows_a + rows_b, HEAD), f32)
    done = pl.pallas_call(
        functools.partial(merge_kernel, len(part_a), len(part_b), (span_a, span_b)),
        out_shape=[result] * heads,
        in_specs=[VMEM] * (len(part_a) + len(part_b)),
        out_specs=[VMEM] * heads,
        compiler_params=SMALL,
    )(*part_a, *part_b)
    back = exchange([d.astype(f16) for d in done], HEAD_AXIS)
    back = [done[0]] + [b.astype(f32) for b in back[1:]]
    return pl.pallas_call(
        join_heads,
        out_shape=[
            jax.ShapeDtypeStruct((rows_a, HEADS * HEAD), f32),
            jax.ShapeDtypeStruct((rows_b, HEADS * HEAD), f32),
        ],
        in_specs=[SMEM] + [VMEM] * heads,
        out_specs=[VMEM] * 2,
        compiler_params=SMALL,
    )(place, *back)


def solution(mesh):
    torus = Mesh(mesh.devices.reshape(4, 2, 2, 4, 2, 2), AXES)
    placed = P(AXES, None)
    return jax.shard_map(
        both_ways,
        mesh=torus,
        in_specs=(placed,) * 4,
        out_specs=(placed, placed),
        check_vma=False,
    )
```
